128 devices in a mesh: rows: 128 (over y, z, x, core).
Axes of the slice: x: 4, y: 4, z: 4, core: 2. Of those that a mesh axis runs over, the one named last changes fastest.
Arguments:
- p_left: bfloat16 [120, 1048576], P(None, 'rows'), may hold values from -0.5 to 0.5
- phi_right: bfloat16 [120, 1048576], P(None, 'rows'), may hold values from -0.005859375 to 0.005859375
- v_cols: bfloat16 [40, 1048576], P(None, 'rows'), may hold values from -6 to 6
- w_cols: bfloat16 [40, 1048576], P(None, 'rows'), may hold values from -6 to 6
- residual: bfloat16 [1048576], P('rows'), may hold values from -8 to 8, as said below
Outputs:
- update: float32 [1048576], P('rows')
- q_left: bfloat16 [160, 1048576], P(None, 'rows')
- q_right: bfloat16 [160, 1048576], P(None, 'rows')
- rms_norms: float32 [2], replicated
The draws below stay inside these ranges and needn't reach their ends.
Inputs may be any that keep to these rules, and one draw needn't show every extreme that they name: A residual that lies mostly in the span of the rows of v_cols.
All inputs are finite; a program needn't handle non-finite values.
Results may differ from the reference program's by a relative error of at most 0.0039.
Values may be sent and summed in bfloat16 or wider, within the bound.
A program may use at most 128 MiB of HBM per device.

```python
import jax
import jax.numpy as jnp
from jax import lax

MDEV = 8192
COLS = 40
RANK = 120
CROSS = 160
MROWS = 1048576
N_ROWS = 128


def blended_rows(key, count):
    own = jnp.clip(jax.random.normal(jax.random.fold_in(key, 1), (count, MROWS), jnp.float32), -5.0, 5.0)
    commons = jnp.clip(jax.random.normal(jax.random.fold_in(key, 2), (4, MROWS), jnp.float32), -5.0, 5.0)
    own_share = 0.6
    loads = jax.random.normal(jax.random.fold_in(key, 3), (count, 4), jnp.float32)
    loads = loads / jnp.sqrt(jnp.sum(loads * loads, axis=1, keepdims=True) + 1e-06)
    shared = jnp.dot(loads, commons)
    common_share = jnp.sqrt(1.0 - own_share * own_share)
    return own_share * own + common_share * shared


def paired_columns(key):
    base = jnp.clip(blended_rows(jax.random.fold_in(key, 11), COLS), -6.0, 6.0)
    weights = jnp.clip(jax.random.normal(jax.random.fold_in(key, 12), (COLS,), jnp.float32), -3.0, 3.0)
    noise = jnp.clip(jax.random.normal(jax.random.fold_in(key, 13), (MROWS,), jnp.float32), -6.0, 6.0)
    mixed = jnp.dot(weights, base) / jnp.sqrt(jnp.float32(COLS)) + 0.3 * noise
    mixed = mixed / jnp.sqrt(jnp.mean(mixed * mixed) + 1e-06)
    return (base, jnp.clip(mixed, -8.0, 8.0))


def draw_v_cols(key, part):
    return paired_columns(key)[0].astype(jnp.bfloat16)


def draw_residual(key, part):
    return paired_columns(key)[1].astype(jnp.bfloat16)


def draw_p_left(key, part):
    rows = blended_rows(jax.random.fold_in(key, 21), RANK) / jnp.sqrt(jnp.float32(RANK))
    return jnp.clip(rows, -0.5, 0.5).astype(jnp.bfloat16)


def draw_phi_right(key, part):
    scale = 1.0 / jnp.sqrt(jnp.float32(MROWS))
    rows = blended_rows(jax.random.fold_in(key, 31), RANK) * scale
    return jnp.clip(rows, -6.0 * scale, 6.0 * scale).astype(jnp.bfloat16)


def block_scale(rng, shape, shards, low, high):
    gain = 1.0
    for axis_at, blocks in shards:
        steps = jax.random.uniform(jax.random.fold_in(jax.random.fold_in(rng, 6), axis_at), (blocks,), jnp.float32, low / len(shards), high / len(shards))
        gain = gain * jnp.repeat(jnp.exp(steps), shape[axis_at] // blocks).reshape((-1,) + (1,) * (len(shape) - 1 - axis_at))
    return gain


def centred(key, shape, spread, most, split=(), kind=jnp.bfloat16):
    loudness = block_scale(key, shape, split, -0.22, 0.18) if split else 1.0
    values = jax.random.normal(key, shape, jnp.float32) * spread * loudness
    return jnp.minimum(jnp.maximum(values, -most), most).astype(kind)


def setup_inputs(seed: int = 0) -> dict:
    keys = jax.random.split(jax.random.key(seed), 6)
    return {
        "p_left": draw_p_left(jax.random.fold_in(keys[5], 71), 0),
        "phi_right": draw_phi_right(jax.random.fold_in(keys[5], 71), 0),
        "v_cols": draw_v_cols(jax.random.fold_in(keys[5], 71), 0),
        "w_cols": centred(keys[3], (COLS, MROWS), 1.0, 6.0, ((1, 128),)),
        "residual": draw_residual(jax.random.fold_in(keys[5], 71), 0),
    }


def lower_solve(factor, rhs, transposed=False):
    return lax.linalg.triangular_solve(factor, rhs, left_side=True, lower=True, transpose_a=transposed)

def split_blocks(array):
    return array.reshape(array.shape[0], N_ROWS, MDEV).transpose(1, 0, 2)

def reference(p_left, phi_right, v_cols, w_cols, residual):
    single = jnp.float32
    half = jnp.bfloat16
    highest = lax.Precision.HIGHEST
    col_gram = jnp.dot(v_cols, v_cols.T, preferred_element_type=single)
    col_res = jnp.dot(v_cols, residual, preferred_element_type=single)
    phi_cols = jnp.dot(phi_right, v_cols.T, preferred_element_type=single)
    phi_res = jnp.dot(phi_right, residual, preferred_element_type=single)
    res_sq = jnp.dot(residual, residual, preferred_element_type=single)
    col_chol = jnp.linalg.cholesky(col_gram)
    coeffs = -lower_solve(col_chol, lower_solve(col_chol, col_res[:, None]), True)[:, 0]
    mix_half = phi_cols.astype(half)
    res_half = phi_res.astype(half)

    def section(pieces):
        p_blk, phi_blk, v_blk, w_blk = pieces
        w_tilde = w_blk.astype(single) - jnp.dot(mix_half.T, p_blk, preferred_element_type=single)
        upd = jnp.dot(coeffs, w_tilde, precision=highest) - jnp.dot(res_half, p_blk, preferred_element_type=single)
        left = jnp.concatenate([p_blk.astype(single), lower_solve(col_chol, w_tilde)], 0)
        right = jnp.concatenate([phi_blk.astype(single), lower_solve(col_chol, v_blk.astype(single))], 0)
        return (upd, left, right)
    blocks = (split_blocks(p_left), split_blocks(phi_right), split_blocks(v_cols), split_blocks(w_cols))

    def first_pass(carry, pieces):
        upd, left, right = section(pieces)
        left_acc = carry[0] + jnp.dot(left, left.T, precision=highest)
        right_acc = carry[1] + jnp.dot(right, right.T, precision=highest)
        upd_acc = carry[2] + jnp.sum(upd * upd)
        return ((left_acc, right_acc, upd_acc), upd)
    start = (jnp.zeros((CROSS, CROSS), single), jnp.zeros((CROSS, CROSS), single), jnp.zeros((), single))
    (left_gram, right_gram, upd_sq), upd_blocks = lax.scan(first_pass, start, blocks)
    left_chol = jnp.linalg.cholesky(left_gram)
    right_chol = jnp.linalg.cholesky(right_gram)

    def second_pass(pieces):
        upd, left, right = section(pieces)
        return (lower_solve(left_chol, left).astype(half), lower_solve(right_chol, right).astype(half))
    left_blocks, right_blocks = lax.map(second_pass, blocks)
    update = upd_blocks.reshape(MROWS)
    q_right = right_blocks.transpose(1, 0, 2).reshape(CROSS, MROWS)
    left_full = left_blocks.transpose(1, 0, 2).reshape(CROSS, MROWS)
    q_left = left_full.reshape(CROSS, MDEV, N_ROWS).transpose(0, 2, 1).reshape(CROSS, MROWS)
    rms_norms = jnp.sqrt(jnp.stack([res_sq, upd_sq]) / MROWS)
    return (update, q_left, q_right, rms_norms)
```

```python
import jax
import jax.numpy as jnp
from jax import lax
from jax.experimental import pallas as pl
from jax.experimental.pallas import tpu as pltpu
from jax.sharding import Mesh
from jax.sharding import PartitionSpec as P

AXES = ("y", "z", "x", "c")
MESH = pl.DeviceIdType.MESH
F32 = jnp.float32
HALF = jnp.bfloat16
HIGHEST = lax.Precision.HIGHEST

RANK, COLS, CROSS = 120, 40, 160
MDEV, DEVS, PLANE = 8192, 128, 32
LANES, TURNS = 128, MDEV // 128
SLAB = 10
PACKED = PLANE * SLAB
STEP_MAIN, STEP_REST = 72, 24
SPREAD = 37
BATCHES = (20, 30, 55)


def mm(a, b):
    return jnp.dot(a, b, precision=HIGHEST, preferred_element_type=F32)


def mt(a, b):
    return lax.dot_general(
        a, b, (((1,), (1,)), ((), ())), precision=HIGHEST, preferred_element_type=F32
    )


def half_mt(a, b):
    return lax.dot_general(a, b, (((1,), (1,)), ((), ())), preferred_element_type=F32)


def iota(shape, dim):
    return lax.broadcasted_iota(jnp.int32, shape, dim)


def tall(rows):
    spare = LANES - rows.shape[0]
    return jnp.concatenate([rows, jnp.zeros((spare, LANES), F32)], 0) if spare else rows


def symmetric(lower):
    square = tall(lower)
    full = jnp.where(iota((LANES, LANES), 1) > iota((LANES, LANES), 0), square.T, square)
    return full[: lower.shape[0]]


def inverse_factors(blocks):
    lane = iota((COLS, LANES), 1)
    row = iota((COLS, LANES), 0)
    unit = jnp.where(lane - COLS == row, 1.0, 0.0).astype(F32)
    work = []
    for block in blocks:
        wide = jnp.concatenate([block, jnp.zeros((COLS, LANES - COLS), F32)], 1)
        wide = jnp.where(lane < COLS, wide, unit)
        work.append([wide[8 * t : 8 * t + 8] for t in range(COLS // 8)])
    inner = iota((8, 1), 0)
    for j in range(COLS - 1):
        t0, s = divmod(j, 8)
        for rows in work:
            line = rows[t0][s : s + 1]
            scaled = line / rows[t0][s : s + 1, j : j + 1]
            for t in range(t0, COLS // 8):
                col = rows[t][:, j : j + 1]
                if t == t0:
                    if s == 7:
                        continue
                    col = jnp.where(inner > s, col, 0.0)
                rows[t] = rows[t] - col * scaled
    out = []
    for rows in work:
        whole = jnp.concatenate(rows, 0)
        pivots = jnp.sum(jnp.where(lane == row, whole, 0.0), 1, keepdims=True)
        whole = whole * lax.rsqrt(pivots)
        out.append(whole[:, COLS : 2 * COLS])
    return out


def coords():
    return tuple(lax.axis_index(a) for a in AXES)


def flat(y, z, x, c):
    return ((y * 4 + z) * 4 + x) * 2 + c


def moved_by(at, o):
    y, z, x, c = at
    return ((y + o // 32) % 4, (z + (o // 8) % 4) % 4, (x + (o // 2) % 4) % 4, (c + o % 2) % 2)


def exchange_kernel(
    p_hbm, phi_hbm, v_hbm, w_hbm, r_ref,
    recv_hbm, xr_hbm, tl_ref, tr_ref, upd_ref, rms_ref,
    pv, phv, vv, wv, xl, xr, st_main, st_rest, sb, gl, gr, g2, gs, gin, g1, ga,
    lsem, s1, r1, s2, r2, s3, r3, sbulk, rbulk, sown, sxr,
):
    at = coords()
    y, z, x, c = at
    me = flat(*at)
    q = (z * 4 + x) * 2 + c

    loads = []
    for n, (src, dst) in enumerate(((p_hbm, pv), (w_hbm, wv), (phi_hbm, phv), (v_hbm, vv))):
        loads.append(pltpu.make_async_copy(src, dst, lsem.at[n]))
        loads[-1].start()

    barrier = pltpu.get_barrier_semaphore()

    def greet(o, _):
        pl.semaphore_signal(barrier, inc=1, device_id=moved_by(at, o), device_id_type=MESH)
        return 0

    lax.fori_loop(1, DEVS, greet, 0)

    wide = 1024
    gl[...] = jnp.zeros_like(gl)
    gr[...] = jnp.zeros_like(gr)
    loads[0].wait()
    loads[1].wait()

    def left_gram(i, _):
        at_cols = pl.ds(pl.multiple_of(i * wide, wide), wide)
        rows = jnp.concatenate([pv[:, at_cols].astype(F32), wv[:, at_cols].astype(F32)], 0).astype(HALF)
        xl[:, at_cols] = rows
        gl[...] += half_mt(rows, rows)
        return 0

    lax.fori_loop(0, MDEV // wide, left_gram, 0)
    loads[2].wait()
    loads[3].wait()

    def right_gram(i, _):
        at_cols = pl.ds(pl.multiple_of(i * wide, wide), wide)
        res = r_ref[pl.ds(pl.multiple_of(i * 8, 8), 8), :].astype(F32)
        line = jnp.concatenate([res[k : k + 1] for k in range(8)], 1)
        both = jnp.concatenate([phv[:, at_cols].astype(F32), vv[:, at_cols].astype(F32)], 0)
        xr[:, at_cols] = both.astype(HALF)
        rows = jnp.concatenate([both, jnp.broadcast_to(line, (8, wide))], 0).astype(HALF)
        gr[...] += half_mt(rows, rows)
        return 0

    lax.fori_loop(0, MDEV // wide, right_gram, 0)
    keep_xr = pltpu.make_async_copy(xr, xr_hbm, sxr)
    keep_xr.start()

    g2[...] = jnp.zeros_like(g2)
    g2[0:96, :] = gl[64:160, 0:128]
    g2[96:192, :] = gr[64:160, 0:128]
    g2[192:256, 0:64] = gl[0:64, 0:64]
    g2[192:256, 64:128] = gr[0:64, 0:64]
    g2[256:288, 0:32] = gl[128:160, 128:160]
    g2[256:288, 32:64] = gr[128:160, 128:160]
    g2[288:296, :] = gr[160:168, 0:128]
    g2[296:304, 0:40] = gr[160:168, 128:168]
    for i in range(PLANE):
        gs[i] = g2[SLAB * i : SLAB * i + SLAB, :]

    pl.semaphore_wait(barrier, DEVS - 1)

    def plane_peer(o):
        return moved_by(at, o)

    def scatter(o, _):
        dev = plane_peer(o)
        dq = (dev[1] * 4 + dev[2]) * 2 + dev[3]
        pltpu.make_async_remote_copy(
            src_ref=gs.at[dq], dst_ref=gin.at[q], send_sem=s1, recv_sem=r1,
            device_id=dev, device_id_type=MESH,
        ).start()
        return 0

    lax.fori_loop(1, PLANE, scatter, 0)
    gin[pl.ds(q, 1)] = gs[pl.ds(q, 1)]

    unit = jnp.where(iota((256, 256), 0) == iota((256, 256), 1), 1.0, 0.0).astype(HALF)

    def turn_main(i, _):
        cols = pl.ds(pl.multiple_of(i * 256, 256), 256)
        turned = half_mt(unit, xl[0:128, cols])
        st_main[pl.ds(2 * i, 128, stride=STEP_MAIN), :] = turned[0:128]
        st_main[pl.ds(2 * i + 1, 128, stride=STEP_MAIN), :] = turned[128:256]
        return 0

    lax.fori_loop(0, TURNS // 2, turn_main, 0)

    def turn_rest(j, _):
        parts = [
            xl[128:160, pl.ds(pl.multiple_of((16 * g + j) * 128, 128), 128)] for g in range(4)
        ]
        turned = half_mt(unit[0:128, 0:128], jnp.concatenate(parts, 0))
        st_rest[pl.ds(j, 128, stride=STEP_REST), :] = turned
        return 0

    lax.fori_loop(0, 16, turn_rest, 0)

    def pack(i, _):
        for k in range(4):
            d = i * 4 + k
            at_main = pl.ds(pl.multiple_of(d * STEP_MAIN, 8), 64)
            at_rest = pl.ds(pl.multiple_of(d * STEP_REST, 8), 16)
            sb[d, 0:64, :] = st_main[at_main, :].astype(HALF)
            sb[d, 64:80, :] = st_rest[at_rest, :].astype(HALF)
        return 0

    lax.fori_loop(0, DEVS // 4, pack, 0)

    def send(i, _):
        dev = moved_by(at, (i * SPREAD) % DEVS)
        pltpu.make_async_remote_copy(
            src_ref=sb.at[flat(*dev)], dst_ref=recv_hbm.at[me], send_sem=sbulk, recv_sem=rbulk,
            device_id=dev, device_id_type=MESH,
        ).start()
        return 0

    own = pltpu.make_async_copy(sb.at[me], recv_hbm.at[me], sown)
    own.start()
    lax.fori_loop(1, BATCHES[0], send, 0)

    def landed(buf, count, sem):
        part = buf.at[pl.ds(0, count)]
        pltpu.make_async_copy(part, part, sem).wait()

    landed(gin, PLANE - 1, r1)
    g1[pl.ds(y, 1)] = jnp.sum(gin[...], 0, keepdims=True)

    def across(o, _):
        pltpu.make_async_remote_copy(
            src_ref=g1.at[y], dst_ref=g1.at[y], send_sem=s2, recv_sem=r2,
            device_id=((y + o) % 4, z, x, c), device_id_type=MESH,
        ).start()
        return 0

    lax.fori_loop(1, 4, across, 0)
    lax.fori_loop(BATCHES[0], BATCHES[1], send, 0)
    landed(g1, 3, r2)
    ga[pl.ds(q, 1)] = (g1[0:1] + g1[1:2]) + (g1[2:3] + g1[3:4])

    def spread(o, _):
        pltpu.make_async_remote_copy(
            src_ref=ga.at[q], dst_ref=ga.at[q], send_sem=s3, recv_sem=r3,
            device_id=plane_peer(o), device_id_type=MESH,
        ).start()
        return 0

    lax.fori_loop(1, PLANE, spread, 0)
    lax.fori_loop(BATCHES[1], BATCHES[2], send, 0)
    landed(ga, PLANE - 1, r3)
    lax.fori_loop(BATCHES[2], DEVS, send, 0)

    for i in range(PLANE):
        g2[SLAB * i : SLAB * i + SLAB, :] = ga[i]
    lane40 = iota((COLS, LANES), 1)

    def unpack(lo, top, corner, shift):
        first = symmetric(jnp.concatenate([top, g2[lo : lo + 64, :]], 0))
        last = g2[lo + 64 : lo + 96, :]
        cross = jnp.concatenate([first[RANK:128], last], 0)
        low = jnp.concatenate(
            [pltpu.roll(first[RANK:128], 8, 1),
             jnp.where(lane40[8:] < 8, pltpu.roll(last, 8, 1), pltpu.roll(corner, shift, 1))], 0)
        return first[0:RANK, 0:RANK], cross[:, 0:RANK], symmetric(low)[:, 0:COLS]

    tops = g2[192:256, :]
    corner = g2[256:288, :]
    pp, wp, ww = unpack(0, tops, corner, 8)
    ff, vf, vvg = unpack(96, pltpu.roll(tops, 64, 1), corner, 104)
    res1 = g2[288:296, :]
    res2 = g2[296:304, :]
    res_f = res1[:, 0:RANK].astype(HALF).astype(F32)
    res_v = jnp.where(lane40[0:8] < 8, pltpu.roll(res1, 8, 1), pltpu.roll(res2, 8, 1))[:, 0:COLS]
    res_sq = res2[:, 32:33]
    mix_t = vf.astype(HALF).astype(F32)

    def col(square, b):
        return square[COLS * b :, COLS * b : COLS * b + COLS]

    wt_p = wp - mm(mix_t, pp)
    wt_wt = ww - mt(mix_t, wp) - mt(wt_p, mix_t)
    cinv, lp, lf = inverse_factors([vvg, pp[0:COLS, 0:COLS], ff[0:COLS, 0:COLS]])
    y_p = mm(cinv, wt_p)
    y_y = mt(mm(cinv, wt_wt), cinv)
    z_f = mm(cinv, vf)
    z_z = mt(mm(cinv, vvg), cinv)

    def columns(square, low, last):
        return [
            jnp.concatenate([col(square, b), low[:, COLS * b : COLS * b + COLS]], 0) for b in range(3)
        ] + [last]

    eye = [
        jnp.where(iota((COLS, CROSS), 1) == iota((COLS, CROSS), 0) + COLS * b, 1.0, 0.0).astype(F32)
        for b in range(3)
    ]
    sides = [
        (columns(pp, y_p, y_y), eye + [jnp.concatenate([-mm(cinv, mix_t), cinv], 1)]),
        (columns(ff, z_f, z_z), eye + [jnp.concatenate([jnp.zeros((COLS, RANK), F32), cinv], 1)]),
    ]
    inverses = [lp, lf]
    for b in range(4):
        if b:
            inverses = inverse_factors([cs[b][0:COLS] for cs, _ in sides])
        for (cs, es), inv in zip(sides, inverses):
            es[b] = mm(inv, es[b])
            if b == 3:
                continue
            below = mt(cs[b][COLS:], inv)
            for k in range(b + 1, 4):
                lo = COLS * (k - b - 1)
                cs[k] = cs[k] - mt(below[lo:], below[lo : lo + COLS])
                es[k] = es[k] - mm(below[lo : lo + COLS], es[b])
    for (cs, es), ref in zip(sides, (tl_ref, tr_ref)):
        whole = jnp.concatenate(es, 0)
        high = whole.astype(HALF)
        ref[0:CROSS, 0:CROSS] = high
        ref[CROSS:, 0:CROSS] = (whole - high.astype(F32)).astype(HALF)
    tl_ref[:, CROSS:] = jnp.zeros((2 * CROSS, 256 - CROSS), HALF)

    coeffs = -mm(mt(res_v, cinv), cinv)
    shift = mm(coeffs, mix_t) + res_f
    upd_sq = (
        jnp.sum(mm(coeffs, wt_wt) * coeffs, 1, keepdims=True)
        - 2.0 * jnp.sum(mm(coeffs, wt_p) * res_f, 1, keepdims=True)
        + jnp.sum(mm(res_f, pp) * res_f, 1, keepdims=True)
    )
    both = jnp.where(iota((8, LANES), 1) == 0, res_sq, upd_sq)
    rms_ref[...] = jnp.sqrt(both / (MDEV * DEVS))

    line = jnp.concatenate([-shift, coeffs], 1)
    one = line.astype(HALF).astype(F32)
    two = (line - one).astype(HALF).astype(F32)
    three = line - one - two
    which = iota((8, CROSS), 0)
    terms = jnp.where(which == 0, one, jnp.where(which == 1, two, jnp.where(which == 2, three, 0.0)))
    terms = terms.astype(HALF)

    def updates(i, _):
        cols = pl.ds(pl.multiple_of(i * wide, wide), wide)
        part = jnp.dot(terms, xl[:, cols], preferred_element_type=F32)
        upd_ref[:, cols] = jnp.sum(part, 0, keepdims=True)
        return 0

    lax.fori_loop(0, MDEV // wide, updates, 0)

    landed(gs, PLANE - 1, s1)
    landed(g1, 3, s2)
    landed(ga, PLANE - 1, s3)
    keep_xr.wait()
    own.wait()
    landed(sb, DEVS - 1, sbulk)
    landed(recv_hbm, DEVS - 1, rbulk)


def finish_kernel(recv_ref, xr_ref, tl_ref, tr_ref, upd_in, rms_in, upd_ref, ql_ref, qr_ref, rms_ref):
    sources = recv_ref.shape[0]
    for s in range(0, sources, 4):
        block = recv_ref[s : s + 4]
        main = block[:, 0:64, :].reshape(256, LANES)
        rest = block[:, 64:80, :].reshape(64, LANES).astype(F32)
        turned = [rest] + [pltpu.roll(rest, LANES - 32 * g, 1) for g in range(1, 4)]
        pieces = []
        for k in range(4):
            pieces += [t[16 * k : 16 * k + 16] for t in turned]
        moved = jnp.concatenate([main, jnp.concatenate(pieces, 0).astype(HALF)], 1)
        cols = pl.ds(64 * s, 256)
        left = half_mt(tl_ref[...], moved)
        ql_ref[:, cols] = (left[0:CROSS] + left[CROSS:]).astype(HALF)
        right = jnp.dot(tr_ref[...], xr_ref[:, cols], preferred_element_type=F32)
        qr_ref[:, cols] = (right[0:CROSS] + right[CROSS:]).astype(HALF)
    upd_ref[...] = upd_in[...]
    rms_ref[...] = rms_in[...]


def shards(p_left, phi_right, v_cols, w_cols, residual):
    hbm = pl.BlockSpec(memory_space=pl.ANY)
    vmem = pl.BlockSpec(memory_space=pltpu.VMEM)
    dma = pltpu.SemaphoreType.DMA
    recv, xr, tl, tr, upd, rms = pl.pallas_call(
        exchange_kernel,
        out_shape=(
            jax.ShapeDtypeStruct((DEVS, 80, LANES), HALF),
            jax.ShapeDtypeStruct((CROSS, MDEV), HALF),
            jax.ShapeDtypeStruct((2 * CROSS, 256), HALF),
            jax.ShapeDtypeStruct((2 * CROSS, CROSS), HALF),
            jax.ShapeDtypeStruct((1, MDEV), F32),
            jax.ShapeDtypeStruct((8, LANES), F32),
        ),
        in_specs=[hbm, hbm, hbm, hbm, vmem],
        out_specs=(hbm, hbm, vmem, vmem, vmem, vmem),
        scratch_shapes=[
            pltpu.VMEM((RANK, MDEV), HALF),
            pltpu.VMEM((RANK, MDEV), HALF),
            pltpu.VMEM((COLS, MDEV), HALF),
            pltpu.VMEM((COLS, MDEV), HALF),
            pltpu.VMEM((CROSS, MDEV), HALF),
            pltpu.VMEM((CROSS, MDEV), HALF),
            pltpu.VMEM((DEVS * STEP_MAIN, LANES), F32),
            pltpu.VMEM((DEVS * STEP_REST, LANES), F32),
            pltpu.VMEM((DEVS, 80, LANES), HALF),
            pltpu.VMEM((CROSS, CROSS), F32),
            pltpu.VMEM((CROSS + 8, CROSS + 8), F32),
            pltpu.VMEM((PACKED, LANES), F32),
            pltpu.VMEM((PLANE, SLAB, LANES), F32),
            pltpu.VMEM((PLANE, SLAB, LANES), F32),
            pltpu.VMEM((4, SLAB, LANES), F32),
            pltpu.VMEM((PLANE, SLAB, LANES), F32),
            dma((4,)), dma, dma, dma, dma, dma, dma, dma, dma, dma, dma,
        ],
        compiler_params=pltpu.CompilerParams(
            collective_id=0, has_side_effects=True, vmem_limit_bytes=48 * 1024 * 1024
        ),
        name="exchange",
    )(p_left, phi_right, v_cols, w_cols, residual.reshape(TURNS, LANES))

    blocks = 8
    upd, ql, qr, rms = pl.pallas_call(
        finish_kernel,
        grid=(blocks,),
        out_shape=(
            jax.ShapeDtypeStruct((1, MDEV), F32),
            jax.ShapeDtypeStruct((CROSS, MDEV), HALF),
            jax.ShapeDtypeStruct((CROSS, MDEV), HALF),
            jax.ShapeDtypeStruct((8, LANES), F32),
        ),
        in_specs=[
            pl.BlockSpec((DEVS // blocks, 80, LANES), lambda i: (i, 0, 0)),
            pl.BlockSpec((CROSS, MDEV // blocks), lambda i: (0, i)),
            pl.BlockSpec((2 * CROSS, 256), lambda i: (0, 0)),
            pl.BlockSpec((2 * CROSS, CROSS), lambda i: (0, 0)),
            pl.BlockSpec((1, MDEV // blocks), lambda i: (0, i)),
            pl.BlockSpec((8, LANES), lambda i: (0, 0)),
        ],
        out_specs=(
            pl.BlockSpec((1, MDEV // blocks), lambda i: (0, i)),
            pl.BlockSpec((CROSS, MDEV // blocks), lambda i: (0, i)),
            pl.BlockSpec((CROSS, MDEV // blocks), lambda i: (0, i)),
            pl.BlockSpec((8, LANES), lambda i: (0, 0)),
        ),
        name="finish",
    )(recv, xr, tl, tr, upd, rms)
    return upd.reshape(MDEV), ql, qr, rms[0, 0:2]


def solution(mesh):
    torus = Mesh(mesh.devices.reshape(4, 4, 4, 2), AXES)
    in_specs = (P(None, AXES), P(None, AXES), P(None, AXES), P(None, AXES), P(AXES))
    out_specs = (P(AXES), P(None, AXES), P(None, AXES), P())
    return jax.shard_map(
        shards, mesh=torus, in_specs=in_specs, out_specs=out_specs, check_vma=False
    )
```
